32 devices in a mesh: tp: 4 (over y, core), dp: 8 (over z, x).
Axes of the slice: x: 2, y: 2, z: 4, core: 2. Of those that a mesh axis runs over, the one named last changes fastest.
Arguments:
- teacher_query: bfloat16 [8192, 8192], P('dp', 'tp'), may hold values from -8 to 8
- student_hidden: bfloat16 [8192, 4096], P('dp', 'tp'), may hold values from -16 to 16
- query_weight: bfloat16 [4096, 4096], P('dp', 'tp'), may hold values from -0.039794922 to 0.039794922
Outputs:
- kl_rows: float32 [32, 8192], P(('tp', 'dp'))
- weight_grad: float32 [4096, 4096], P('dp', 'tp')
The draws below stay inside these ranges and needn't reach their ends.
All inputs are finite; a program needn't handle non-finite values.
Results may differ from the reference program's by a relative error of at most 0.0029.
Values may be sent and summed in bfloat16 or wider, within the bound.
A program may use at most 64 MiB of HBM per device.

```python
import jax
import jax.numpy as jnp
from jax import lax

DT = 8192
DS = 4096
RHEADS = 32
NSEQ = 2
SEQ = 4096
QBLOCKS = 1
QROWS = 4096


def draw_teacher_query(key, part):
    values = 0.5 * jnp.clip(jax.random.normal(jax.random.fold_in(key, 1), (NSEQ * SEQ, DT), jnp.float32), -4.0, 4.0)
    return values.astype(jnp.bfloat16)


def draw_student_hidden(key, part):
    values = jnp.clip(jax.random.normal(jax.random.fold_in(key, 2), (NSEQ * SEQ, DS), jnp.float32), -4.0, 4.0)
    return values.astype(jnp.bfloat16)


def steps_of(rng, dims, cuts, smallest, largest):
    def one(position, parts):
        heights = jax.random.uniform(jax.random.fold_in(jax.random.fold_in(rng, 6), position), (parts,), jnp.float32, smallest / len(cuts), largest / len(cuts))
        return jnp.repeat(jnp.exp(heights), dims[position] // parts).reshape((-1,) + (1,) * (len(dims) - position - 1))

    factor_of = one(*cuts[0])
    for cut in cuts[1:]:
        factor_of = factor_of * one(*cut)
    return factor_of


def noise(stream_key, shape, scale, bound, shards=(), held_as=jnp.bfloat16):
    drawn = jax.random.normal(stream_key, shape, jnp.float32) * scale
    if len(shards) > 0:
        drawn = steps_of(stream_key, shape, shards, -0.22, 0.18) * drawn
    return jnp.clip(drawn, min=-bound, max=bound).astype(held_as)


def setup_inputs(seed: int = 0) -> dict:
    arg_keys = jax.random.split(jax.random.key(seed), 4)
    return {
        "teacher_query": draw_teacher_query(jax.random.fold_in(arg_keys[3], 71), 0),
        "student_hidden": draw_student_hidden(jax.random.fold_in(arg_keys[3], 71), 0),
        "query_weight": noise(arg_keys[2], (DS, DS), 0.0078125, 0.039794922, ((0, 8), (1, 4))),
    }


def head_terms(pair):
    teacher_head, student_head = pair
    teacher_scale = teacher_head.shape[1] ** -0.5
    student_scale = student_head.shape[1] ** -0.5
    teacher_scores = lax.dot_general(teacher_head, teacher_head, (((1,), (1,)), ((), ())), preferred_element_type=jnp.float32) * teacher_scale
    student_scores = lax.dot_general(student_head, student_head, (((1,), (1,)), ((), ())), preferred_element_type=jnp.float32) * student_scale
    teacher_log = jax.nn.log_softmax(teacher_scores, axis=-1)
    student_log = jax.nn.log_softmax(student_scores, axis=-1)
    teacher_prob = jnp.exp(teacher_log)
    divergence = jnp.sum(teacher_prob * (teacher_log - student_log), axis=-1)
    score_grad = (jnp.exp(student_log) - teacher_prob).astype(jnp.bfloat16)
    row_part = jnp.dot(score_grad, student_head, preferred_element_type=jnp.float32)
    key_part = lax.dot_general(score_grad, student_head, (((0,), (0,)), ((), ())), preferred_element_type=jnp.float32)
    return divergence, (row_part + key_part) * student_scale


def reference(teacher_query, student_hidden, query_weight):
    student_query = jnp.dot(student_hidden, query_weight, preferred_element_type=jnp.float32).astype(jnp.bfloat16)
    teacher_width = DT // RHEADS
    student_width = DS // RHEADS
    teacher_heads = teacher_query.reshape(NSEQ, SEQ, RHEADS, teacher_width).transpose(2, 0, 1, 3).reshape(RHEADS * NSEQ, SEQ, teacher_width)
    student_heads = student_query.reshape(NSEQ, SEQ, RHEADS, student_width).transpose(2, 0, 1, 3).reshape(RHEADS * NSEQ, SEQ, student_width)
    divergence, head_grads = lax.map(head_terms, (teacher_heads, student_heads))
    query_grad = head_grads.reshape(RHEADS, NSEQ, SEQ, student_width).transpose(1, 2, 0, 3).reshape(NSEQ * SEQ, DS).astype(jnp.bfloat16)
    weight_grad = lax.dot_general(student_hidden, query_grad, (((0,), (0,)), ((), ())), preferred_element_type=jnp.float32)
    kl_rows = divergence.reshape(RHEADS, NSEQ, QBLOCKS, QROWS).transpose(0, 2, 1, 3).reshape(RHEADS * QBLOCKS, NSEQ * QROWS)
    return kl_rows, weight_grad
```

```python
import functools
import math

import jax
import jax.numpy as jnp
from jax import lax
from jax.experimental import pallas as pl
from jax.experimental.pallas import tpu as pltpu
from jax.sharding import PartitionSpec as P

RHEADS = 32
NSEQ = 2
SEQ = 4096


def spread_heads(queries, heads, copies):
    rows = queries.shape[0]
    width = queries.shape[1] // heads
    shaped = queries.reshape(rows, heads, 1, width)
    return jnp.broadcast_to(shaped, (rows, heads, copies, width)).reshape(
        rows, heads * copies, width
    )

LOG2E = 1.0 / math.log(2.0)
LN2 = math.log(2.0)
LANES = 128


def relation_body(
    t_rows, t_keys, s_rows, s_keys, s_rows_t, kl_out, grad_out, t_buf, s_buf, g_buf, row_acc, key_acc,
    *, group, chunk, t_scale, s_scale,
):
    step = pl.program_id(0)
    block = t_rows.shape[0]
    keys = t_keys.shape[0]
    nt = (((1,), (1,)), ((), ()))

    for c in range(keys // chunk):
        at = slice(c * chunk, (c + 1) * chunk)
        t_buf[:, at] = lax.dot_general(t_rows[...], t_keys[at, :], nt, preferred_element_type=jnp.float32)
        s_buf[:, at] = lax.dot_general(s_rows[...], s_keys[at, :], nt, preferred_element_type=jnp.float32)

    tiles = keys // LANES
    ct = t_scale * LOG2E
    cs = s_scale * LOG2E

    def rows_of(i, carry):
        at = pl.ds(pl.multiple_of(i * group, group), group)
        t_max = t_buf[at, 0:LANES]
        s_max = s_buf[at, 0:LANES]
        for k in range(1, tiles):
            cols = slice(k * LANES, (k + 1) * LANES)
            t_max = jnp.maximum(t_max, t_buf[at, cols])
            s_max = jnp.maximum(s_max, s_buf[at, cols])
        t_max = jnp.broadcast_to(jnp.max(t_max, axis=1, keepdims=True), (group, LANES))
        s_max = jnp.broadcast_to(jnp.max(s_max, axis=1, keepdims=True), (group, LANES))
        t_sum = jnp.zeros((group, LANES), jnp.float32)
        s_sum = jnp.zeros((group, LANES), jnp.float32)
        gap = jnp.zeros((group, LANES), jnp.float32)
        for k in range(tiles):
            cols = slice(k * LANES, (k + 1) * LANES)
            u = (t_buf[at, cols] - t_max) * ct
            v = (s_buf[at, cols] - s_max) * cs
            t_exp = jnp.exp2(u)
            s_exp = jnp.exp2(v)
            t_buf[at, cols] = t_exp
            s_buf[at, cols] = s_exp
            t_sum = t_sum + t_exp
            s_sum = s_sum + s_exp
            gap = gap + t_exp * (u - v)
        t_sum = jnp.sum(t_sum, axis=1, keepdims=True)
        s_sum = jnp.sum(s_sum, axis=1, keepdims=True)
        gap = jnp.sum(gap, axis=1, keepdims=True)
        kl = gap * LN2 / t_sum - jnp.log(t_sum) + jnp.log(s_sum)
        kl_out[0, at, :] = jnp.broadcast_to(kl, (group, LANES))
        t_inv = jnp.broadcast_to(1.0 / t_sum, (group, LANES))
        s_inv = jnp.broadcast_to(1.0 / s_sum, (group, LANES))
        for k in range(tiles):
            cols = slice(k * LANES, (k + 1) * LANES)
            g_buf[at, cols] = (s_buf[at, cols] * s_inv - t_buf[at, cols] * t_inv).astype(jnp.bfloat16)
        return carry

    lax.fori_loop(0, block // group, rows_of, 0)

    @pl.when(step == 0)
    def _():
        key_acc[...] = jnp.zeros_like(key_acc)

    row_acc[pl.ds(pl.multiple_of(step * block, block), block), :] = jnp.dot(
        g_buf[...], s_keys[...], preferred_element_type=jnp.float32
    )
    for c in range(keys // chunk):
        at = slice(c * chunk, (c + 1) * chunk)
        key_acc[:, at] += jnp.dot(s_rows_t[...], g_buf[:, at], preferred_element_type=jnp.float32)

    @pl.when(step == pl.num_programs(0) - 1)
    def _():
        def finish(c, carry):
            at = pl.ds(pl.multiple_of(c * LANES, LANES), LANES)
            grad_out[at, :] = ((row_acc[at, :] + key_acc[:, at].T) * s_scale).astype(jnp.bfloat16)
            return carry

        lax.fori_loop(0, keys // LANES, finish, 0)


def relation(teacher, student):
    keys, t_width = teacher.shape
    s_width = student.shape[1]
    block = min(256, keys)
    group = 16
    chunk = min(1024, keys)
    steps = keys // block
    kl, grad = pl.pallas_call(
        functools.partial(
            relation_body, group=group, chunk=chunk, t_scale=t_width ** (-0.5), s_scale=s_width ** (-0.5)
        ),
        grid=(steps,),
        in_specs=[
            pl.BlockSpec((block, t_width), lambda i: (i, 0)),
            pl.BlockSpec((keys, t_width), lambda i: (0, 0)),
            pl.BlockSpec((block, s_width), lambda i: (i, 0)),
            pl.BlockSpec((keys, s_width), lambda i: (0, 0)),
            pl.BlockSpec((s_width, block), lambda i: (0, i)),
        ],
        out_specs=[
            pl.BlockSpec((1, block, LANES), lambda i: (i, 0, 0)),
            pl.BlockSpec((keys, s_width), lambda i: (0, 0)),
        ],
        out_shape=[
            jax.ShapeDtypeStruct((steps, block, LANES), jnp.float32),
            jax.ShapeDtypeStruct((keys, s_width), jnp.bfloat16),
        ],
        scratch_shapes=[
            pltpu.VMEM((block, keys), jnp.float32),
            pltpu.VMEM((block, keys), jnp.float32),
            pltpu.VMEM((block, keys), jnp.bfloat16),
            pltpu.VMEM((keys, s_width), jnp.float32),
            pltpu.VMEM((s_width, keys), jnp.float32),
        ],
        compiler_params=pltpu.CompilerParams(
            dimension_semantics=("arbitrary",), vmem_limit_bytes=40 * 1024 * 1024
        ),
        name="relation",
    )(teacher, teacher, student, student, student.T)
    return kl[:, :, 0].reshape(keys), grad


def whole_heads(teacher_query, student_hidden, query_weight):
    width = teacher_query.shape[1] // lax.axis_size("dp")
    teacher_all = lax.all_to_all(teacher_query, "dp", split_axis=1, concat_axis=0, tiled=True)
    hidden_full = lax.all_gather(student_hidden, "tp", axis=1, tiled=True)
    weight_full = lax.all_gather(query_weight, "dp", axis=0, tiled=True)
    student_query = jnp.dot(hidden_full, weight_full, preferred_element_type=jnp.float32).astype(jnp.bfloat16)
    student_all = lax.all_to_all(student_query, "dp", split_axis=1, concat_axis=0, tiled=True)
    hidden_cols = lax.all_to_all(hidden_full, "dp", split_axis=1, concat_axis=0, tiled=True)
    kls = []
    total = None
    for s in range(NSEQ):
        at = slice(s * SEQ, (s + 1) * SEQ)
        kl, grad = relation(teacher_all[at], student_all[at])
        kls.append(kl)
        grads = lax.all_gather(grad, "dp", axis=1, tiled=True)
        part = lax.dot_general(
            hidden_cols[at], grads, (((0,), (0,)), ((), ())), preferred_element_type=jnp.float32
        )
        total = part if total is None else total + part
    return jnp.concatenate(kls).reshape(1, NSEQ * SEQ), total


def local(teacher_query, student_hidden, query_weight):
    heads_here = RHEADS // lax.axis_size("tp")
    copies = lax.axis_size("dp") // heads_here
    if copies == 1 and heads_here == lax.axis_size("dp"):
        return whole_heads(teacher_query, student_hidden, query_weight)
    rows = teacher_query.shape[0]
    teacher_width = teacher_query.shape[1] // heads_here
    hidden_full = lax.all_gather(student_hidden, "tp", axis=1, tiled=True)
    teacher_send = spread_heads(teacher_query, heads_here, copies)
    projected = jnp.dot(
        hidden_full,
        lax.all_gather(query_weight, "dp", axis=0, tiled=True),
        preferred_element_type=jnp.float32,
    )
    student_query = projected.astype(jnp.bfloat16)
    student_width = student_query.shape[1] // heads_here
    student_send = spread_heads(student_query, heads_here, copies)
    teacher_all, student_all = (
        lax.all_to_all(teacher_send, "dp", split_axis=1, concat_axis=0, tiled=True),
        lax.all_to_all(student_send, "dp", split_axis=1, concat_axis=0, tiled=True),
    )
    total_rows = teacher_all.shape[0]
    teacher_all = teacher_all.reshape(total_rows, teacher_width)
    student_all = student_all.reshape(total_rows, student_width)
    teacher_scale = teacher_width ** (-0.5)
    student_scale = student_width ** (-0.5)
    query_rows = SEQ // copies
    first_row = lax.axis_index("dp") % copies * query_rows
    block = min(512, query_rows)
    blocks_each = query_rows // block

    def relation_step(step, carry):
        kl_store, grad_store = carry
        sequence = step // blocks_each
        offset = step % blocks_each * block
        base = sequence * SEQ
        start = base + first_row + offset
        teacher_keys = lax.dynamic_slice_in_dim(teacher_all, base, SEQ, 0)
        student_keys = lax.dynamic_slice_in_dim(student_all, base, SEQ, 0)
        teacher_rows = lax.dynamic_slice_in_dim(teacher_all, start, block, 0)
        student_rows = lax.dynamic_slice_in_dim(student_all, start, block, 0)
        teacher_scores = (
            lax.dot_general(
                teacher_rows,
                teacher_keys,
                (((1,), (1,)), ((), ())),
                preferred_element_type=jnp.float32,
            )
            * teacher_scale
        )
        student_scores = (
            lax.dot_general(
                student_rows,
                student_keys,
                (((1,), (1,)), ((), ())),
                preferred_element_type=jnp.float32,
            )
            * student_scale
        )
        teacher_log = jax.nn.log_softmax(teacher_scores, axis=-1)
        student_log = jax.nn.log_softmax(student_scores, axis=-1)
        teacher_prob = jnp.exp(teacher_log)
        divergence = jnp.sum(teacher_prob * (teacher_log - student_log), axis=-1)
        score_grad = (jnp.exp(student_log) - teacher_prob).astype(jnp.bfloat16)
        key_part = (
            lax.dot_general(
                score_grad,
                student_rows,
                (((0,), (0,)), ((), ())),
                preferred_element_type=jnp.float32,
            )
            * student_scale
        )
        row_part = (
            jnp.dot(score_grad, student_keys, preferred_element_type=jnp.float32) * student_scale
        )
        seq_grad = lax.dynamic_slice_in_dim(grad_store, base, SEQ, 0)
        grad_store = lax.dynamic_update_slice_in_dim(grad_store, seq_grad + key_part, base, 0)
        current = lax.dynamic_slice_in_dim(grad_store, start, block, 0)
        grad_store = lax.dynamic_update_slice_in_dim(grad_store, current + row_part, start, 0)
        kl_store = lax.dynamic_update_slice_in_dim(
            kl_store, divergence, sequence * query_rows + offset, 0
        )
        return (kl_store, grad_store)

    kl_init = jnp.zeros((NSEQ * query_rows,), jnp.float32)
    grad_init = jnp.zeros((total_rows, student_width), jnp.float32)
    kl_store, grad_store = lax.fori_loop(0, NSEQ * blocks_each, relation_step, (kl_init, grad_init))
    returned = lax.all_to_all(
        grad_store.reshape(heads_here * copies, rows, student_width),
        "dp",
        split_axis=0,
        concat_axis=2,
        tiled=True,
    )
    summed = jnp.sum(returned.reshape(rows, heads_here, copies, student_width), axis=2)
    query_grad = summed.reshape(rows, heads_here * student_width).astype(jnp.bfloat16)
    weight_grad = lax.psum_scatter(
        lax.dot_general(
            hidden_full, query_grad, (((0,), (0,)), ((), ())), preferred_element_type=jnp.float32
        ),
        "dp",
        scatter_dimension=0,
        tiled=True,
    )
    return (kl_store.reshape(1, NSEQ * query_rows), weight_grad)


def solution(mesh):
    placed = (P("dp", "tp"), P("dp", "tp"), P("dp", "tp"))
    return jax.shard_map(
        local,
        mesh=mesh,
        in_specs=placed,
        out_specs=(P(("tp", "dp"), None), P("dp", "tp")),
        check_vma=False,
    )
```
